128 devices in a mesh: row: 2 (over x_lo), col: 64 (over z, y, x_hi, core).
Axes of the slice: x: 4 (x_hi: 2, x_lo: 2; x = x_hi * 2 + x_lo), y: 4, z: 4, core: 2. Of those that a mesh axis runs over, the one named last changes fastest.
Arguments:
- panel: bfloat16 [196608, 1024], P('col', 'row'), may hold values from -0.1875 to 0.1875
- rhs: float32 [1024, 196608], P('row', 'col'), may hold values from -6 to 6
- diag_inverse: bfloat16 [2, 512, 512], replicated, may hold values from -1 to 2, as said below
Outputs:
- solved: bfloat16 [1024, 1024], P(None, 'row')
- updated: float32 [1024, 196608], P('row', 'col')
The draws below stay inside these ranges and needn't reach their ends.
Inputs may be any that keep to these rules, and one draw needn't show every extreme that they name: `diag_inverse`: each block is lower triangular; its diagonal entries are 0.5 or more.
All inputs are finite; a program needn't handle non-finite values.
Results may differ from the reference program's by a relative error of at most 0.0065.
Values may be sent and summed in bfloat16 or wider, within the bound.
No kernel may reach another device: no remote copies, remote signals or barrier semaphores. Data moves between devices by JAX's collectives and lax.ppermute only.
A program may use at most 128 MiB of HBM per device.

```python
import jax
import jax.numpy as jnp
from jax import lax

NB = 512
NBR_DEV = 6
NRHS = 1024
STEPS = 2
N = 196608


def draw_diag_inverse(key, part):
    base = jax.random.fold_in(key, 11)
    first_key, second_key = jax.random.split(base)
    spread = jnp.clip(jax.random.normal(first_key, (STEPS, NB, NB), jnp.float32), -3.0, 3.0)
    diagonal = jax.random.uniform(second_key, (STEPS, NB), jnp.float32, 0.6, 1.6)
    lower = jnp.tril(spread, -1) / jnp.sqrt(jnp.float32(NB))
    whole = lower + jnp.eye(NB, dtype=jnp.float32)[None, :, :] * diagonal[:, :, None]
    return whole.astype(jnp.bfloat16)


def block_levels(stream_key, shape, cuts, smallest, top_value):
    def one(dim, blocks):
        steps = jax.random.uniform(jax.random.fold_in(jax.random.fold_in(stream_key, 6), dim), (blocks,), jnp.float32, smallest / len(cuts), top_value / len(cuts))
        return jnp.repeat(jnp.exp(steps), shape[dim] // blocks).reshape((-1,) + (1,) * (len(shape) - dim - 1))

    gain = one(*cuts[0])
    for cut in cuts[1:]:
        gain = gain * one(*cut)
    return gain


def bell_draw(stream_key, extent, scale, most, cuts=(), held_as=jnp.bfloat16):
    drawn = scale * jax.random.normal(stream_key, extent, jnp.float32)
    if cuts:
        drawn = drawn * block_levels(stream_key, extent, cuts, -0.22, 0.18)
    return jnp.clip(drawn, -most, most).astype(held_as)


def setup_inputs(seed: int = 0) -> dict:
    keys = jax.random.split(jax.random.key(seed), 4)
    panel = bell_draw(keys[0], (N, STEPS * NB), (STEPS * NB) ** -0.5, 0.1875, ((0, 64), (1, 2)))
    rhs = bell_draw(keys[1], (NRHS, N), 1.0, 6.0, ((0, 2), (1, 64)), jnp.float32)
    diag_inverse = draw_diag_inverse(jax.random.fold_in(keys[3], 71), 0)
    return dict(panel=panel, rhs=rhs, diag_inverse=diag_inverse)


def reference(panel, rhs, diag_inverse):
    rows_dev = NBR_DEV * NB
    masked = panel
    for current in range(STEPS):
        start = current * rows_dev
        masked = masked.at[start:start + NB, current * NB:].set(jnp.zeros((), jnp.bfloat16))
    pieces = []
    for current in range(STEPS):
        start = current * rows_dev
        residual = rhs[:, start:start + NB]
        if current > 0:
            earlier = jnp.concatenate(pieces, axis=1)
            factor_rows = masked[start:start + NB, 0:current * NB]
            products = lax.dot_general(earlier, factor_rows, (((1,), (1,)), ((), ())), preferred_element_type=jnp.float32)
            residual = residual - products
        inverse = diag_inverse[current].astype(jnp.float32)
        solution = jnp.dot(residual, inverse.T, precision=lax.Precision.HIGHEST)
        pieces.append(solution.astype(jnp.bfloat16))
    solved = jnp.concatenate(pieces, axis=1)
    window = lax.dot_general(solved, masked, (((1,), (1,)), ((), ())), preferred_element_type=jnp.float32)
    updated = rhs - window
    return solved, updated
```

```python
import functools

import jax
import jax.numpy as jnp
from jax import lax
from jax.experimental import pallas as pl
from jax.experimental.pallas import tpu as pltpu
from jax.sharding import Mesh
from jax.sharding import PartitionSpec as P


NB = 512
COL = ("z", "y", "xh", "core")
ALL = ("row",) + COL
NT = (((1,), (1,)), ((), ()))
F32 = jnp.float32
BF16 = jnp.bfloat16
CUTS = (0, 512, 1024, 1536, 2048, 2560, 3072)
TILE = 256
PARAMS = pltpu.CompilerParams(vmem_limit_bytes=16 << 20)


def dot_nt(a, b):
    return lax.dot_general(a, b, NT, preferred_element_type=F32)


def times_inverse(x, inverse):
    high = x.astype(BF16)
    rest = x - high.astype(F32)
    mid = rest.astype(BF16)
    low = (rest - mid.astype(F32)).astype(BF16)
    return dot_nt(low, inverse) + dot_nt(mid, inverse) + dot_nt(high, inverse)


def first_body(rhs_ref, inv_ref, out_ref):
    out_ref[...] = times_inverse(rhs_ref[...], inv_ref[0]).astype(BF16)


def first_solve(rhs, diag_inverse):
    step = NB // 2
    return pl.pallas_call(
        first_body,
        grid=(2,),
        in_specs=[
            pl.BlockSpec((step, NB), lambda i: (i, 0)),
            pl.BlockSpec((1, NB, NB), lambda i: (0, 0, 0)),
        ],
        out_specs=pl.BlockSpec((step, NB), lambda i: (i, 0)),
        out_shape=jax.ShapeDtypeStruct((NB, NB), BF16),
        compiler_params=PARAMS,
        cost_estimate=pl.CostEstimate(flops=6 * NB**3, bytes_accessed=4 << 20, transcendentals=0),
        name="first_solve",
    )(rhs, diag_inverse)


def second_body(flags, rhs_ref, inv_ref, own_ref, arrived_ref, below_ref, sent_ref, *outs):
    below = jnp.where(flags[0] == 0, below_ref[...], sent_ref[...])
    part = NB // len(outs)
    for q, out in enumerate(outs):
        rows = pl.ds(q * part, part)
        residual = rhs_ref[rows, :] - dot_nt(arrived_ref[rows, :], below)
        second = times_inverse(residual, inv_ref[0]).astype(BF16)
        out[...] = jnp.where(flags[1] == 0, own_ref[rows, :], second)


def second_solve(flags, rhs, diag_inverse, own, arrived, panel, sent):
    whole = pl.BlockSpec((NB, NB), lambda i, f: (0, 0))
    part = pl.BlockSpec((NB // 4, NB), lambda i, f: (0, 0))
    return pl.pallas_call(
        second_body,
        grid_spec=pltpu.PrefetchScalarGridSpec(
            num_scalar_prefetch=1,
            grid=(1,),
            in_specs=[whole, pl.BlockSpec((1, NB, NB), lambda i, f: (1, 0, 0))] + [whole] * 4,
            out_specs=[part] * 4,
        ),
        out_shape=[jax.ShapeDtypeStruct((NB // 4, NB), BF16)] * 4,
        compiler_params=PARAMS,
        cost_estimate=pl.CostEstimate(flops=8 * NB**3, bytes_accessed=4 << 20, transcendentals=0),
        name="second_solve",
    )(flags, rhs, diag_inverse, own, arrived, panel, sent)


def vmem_call(body, flags, operands, outs):
    return pl.pallas_call(
        body,
        in_specs=[pl.BlockSpec(memory_space=pltpu.SMEM)]
        + [pl.BlockSpec(memory_space=pltpu.VMEM)] * len(operands),
        out_specs=[pl.BlockSpec(memory_space=pltpu.VMEM)] * len(outs),
        out_shape=[jax.ShapeDtypeStruct(shape, BF16) for shape in outs],
        compiler_params=PARAMS,
        cost_estimate=pl.CostEstimate(flops=1 << 20, bytes_accessed=1 << 20, transcendentals=0),
    )(flags, *operands)


def ring_body(flags, own, up, down, far, out):
    y = flags[3]
    out[y] = own[...]
    out[lax.rem(y + 1, 4)] = down[...]
    out[lax.rem(y + 2, 4)] = far[...]
    out[lax.rem(y + 3, 4)] = up[...]


def plane_body(flags, own, up, down, far_a, far_b, out):
    z = flags[2]
    for y in range(4):
        rows = slice(y * 32, y * 32 + 32)
        far = far_a if y < 2 else far_b
        for h in range(2):
            out[h, z, rows] = own[y, h]
            out[h, lax.rem(z + 1, 4), rows] = down[y, h]
            out[h, lax.rem(z + 2, 4), rows] = far[y % 2, h]
            out[h, lax.rem(z + 3, 4), rows] = up[y, h]


def finish_body(flags, mine, theirs, solved, left, right):
    row = flags[0]
    same = flags[1] == row
    for h in range(2):
        rows = pl.ds(h * NB, NB)
        solved[rows, :] = jnp.where(same, mine[h], theirs[h])
    left[...] = jnp.where(same, mine[row], theirs[row])
    right[...] = jnp.where(same, theirs[row], mine[row])


def update_body(masks, flags, left, right, rhs, own, other, *rest):
    out = rest[-1]
    first = dot_nt(left[...], own[...])
    if masks:
        arrived = jnp.where(flags[6] == 0, other[...], rest[0][...])
        second = dot_nt(right[...], arrived)
        first = jnp.where(flags[4] == 0, jnp.zeros_like(first), first)
        second = jnp.where(flags[5] == 0, jnp.zeros_like(second), second)
    else:
        second = dot_nt(right[...], other[...])
    out[...] = rhs[...] - (first + second)


def update(flags, left, right, rhs, panel, other, start, stop, before, sent):
    base = start // TILE
    whole = pl.BlockSpec((NB, NB), lambda i, f: (0, 0))
    across = pl.BlockSpec((NB, TILE), lambda i, f: (0, base + i))
    arrived = pl.BlockSpec((TILE, NB), lambda i, f: (i, 0))
    operands = [left, right, rhs, panel, other]
    specs = [whole, whole, across, pl.BlockSpec((TILE, NB), lambda i, f: (base + i, 0)), arrived]
    aliases = {}
    if sent is not None:
        operands.append(sent)
        specs.append(arrived)
    if before is not None:
        aliases = {1 + len(operands): 0}
        operands.append(before)
        specs.append(pl.BlockSpec(memory_space=pl.ANY))
    return pl.pallas_call(
        functools.partial(update_body, sent is not None),
        grid_spec=pltpu.PrefetchScalarGridSpec(
            num_scalar_prefetch=1,
            grid=((stop - start) // TILE,),
            in_specs=specs,
            out_specs=across,
        ),
        out_shape=jax.ShapeDtypeStruct(rhs.shape, F32),
        input_output_aliases=aliases,
        compiler_params=PARAMS,
        cost_estimate=pl.CostEstimate(
            flops=4 * NB * NB * (stop - start), bytes_accessed=4 << 20, transcendentals=0
        ),
        name="update",
    )(flags, *operands)


def shards(panel, rhs, diag_inverse):
    row, z, y, xh, core = (lax.axis_index(name) for name in ALL)
    col = ((z * 4 + y) * 2 + xh) * 2 + core
    window = col < 2
    keep_own = jnp.logical_not(window & (row >= col))
    keep_other = jnp.logical_not(window & (1 - row >= col))
    flags = jnp.stack(
        [a.astype(jnp.int32) for a in (row, core, z, y, keep_own, keep_other, window)]
    )
    swap = [(0, 1), (1, 0)]
    pieces = [panel[a:b] for a, b in zip(CUTS[:-1], CUTS[1:])]

    def shift(value, axis, by):
        return lax.ppermute(value, axis, [(i, (i + by) % 4) for i in range(4)])

    sent = lax.ppermute(pieces[0], ALL, [(1, 65)])
    pairs = [(c, 64 + c) for c in range(2, 64)]
    others = [lax.ppermute(pieces[0], ALL, pairs + [(b, a) for a, b in pairs])]
    for k in range(1, len(pieces)):
        others.append(lax.ppermute(pieces[k], "row", swap))
    first = first_solve(rhs, diag_inverse)
    arrived = lax.ppermute(first, "core", [(0, 1)])
    quarters = second_solve(flags, rhs, diag_inverse, first, arrived, panel, sent)

    got = [lax.ppermute(quarters[q], "z", [(0, q)]) for q in range(1, 4)]
    mine = jnp.where(
        z == 0, quarters[0], jnp.where(z == 1, got[0], jnp.where(z == 2, got[1], got[2]))
    )
    got = [lax.ppermute(mine[32 * q : 32 * q + 32], "y", [(0, q)]) for q in range(1, 4)]
    mine = jnp.where(y == 0, mine[:32], jnp.where(y == 1, got[0], jnp.where(y == 2, got[1], got[2])))
    theirs = lax.ppermute(mine, "row", swap)
    both = jnp.stack([jnp.where(row == 0, mine, theirs), jnp.where(row == 0, theirs, mine)])
    over = lax.ppermute(both, ("row", "xh"), [(2, 1), (0, 3)])
    both = jnp.where(xh == 0, both, over)
    up, down, far = (shift(both, "y", by) for by in (1, -1, 2))
    (line,) = vmem_call(ring_body, flags, [both, up, down, far], [(4, 2, 32, NB)])
    up, down = shift(line, "z", 1), shift(line, "z", -1)
    far_a, far_b = shift(up[:2], "z", 1), shift(down[2:], "z", -1)
    (plane,) = vmem_call(plane_body, flags, [line, up, down, far_a, far_b], [(2, 4, 128, NB)])
    plane = plane.reshape(2, NB, NB)
    theirs = lax.ppermute(plane, "core", swap)
    solved, left, right = vmem_call(
        finish_body, flags, [plane, theirs], [(2 * NB, NB), (NB, NB), (NB, NB)]
    )
    updated = None
    for k, other in enumerate(others):
        updated = update(
            flags, left, right, rhs, panel, other, CUTS[k], CUTS[k + 1], updated,
            sent if k == 0 else None,
        )
    return solved, updated


def solution(mesh):
    split = Mesh(mesh.devices.reshape(2, 4, 4, 2, 2), ALL)
    return jax.shard_map(
        shards,
        mesh=split,
        in_specs=(P(COL, "row"), P("row", COL), P()),
        out_specs=(P(None, "row"), P("row", COL)),
        check_vma=False,
    )
```

```python
import functools

import jax
import jax.numpy as jnp
from jax import lax
from jax.experimental import pallas as pl
from jax.experimental.pallas import tpu as pltpu
from jax.sharding import Mesh
from jax.sharding import PartitionSpec as P


NB = 512
COL = ("z", "y", "xh", "core")
ALL = ("row",) + COL
NT = (((1,), (1,)), ((), ()))
F32 = jnp.float32
BF16 = jnp.bfloat16
CUTS = (0, 512, 1280, 2048, 2560, 2816, 3072)
SIZES = tuple(b - a for a, b in zip(CUTS[:-1], CUTS[1:]))
GROUPS = ((0, 1, 2), (3,), (4,), (5,))
TILE = 256
VMEM_BYTES = 67043328

VMEM = pl.BlockSpec(memory_space=pltpu.VMEM)
HBM = pl.BlockSpec(memory_space=pltpu.HBM)


def column():
    index = lax.axis_index(COL[0])
    for name, size in zip(COL[1:], (4, 2, 2)):
        index = index * size + lax.axis_index(name)
    return index


def dot_nt(a, b):
    return lax.dot_general(a, b, NT, preferred_element_type=F32)


def times_inverse(x, inverse):
    high = x.astype(BF16)
    rest = x - high.astype(F32)
    mid = rest.astype(BF16)
    low = (rest - mid.astype(F32)).astype(BF16)
    parts = dot_nt(jnp.concatenate([low, mid, high], axis=0), inverse)
    count = x.shape[0]
    return parts[:count] + parts[count : 2 * count] + parts[2 * count :]


def call(body, operands, in_specs, outs, scratch=(), flops=1 << 20, room=None):
    limit = 12 << 20 if room is None else VMEM_BYTES - (room << 10)
    return pl.pallas_call(
        body,
        in_specs=in_specs,
        out_specs=[VMEM] * len(outs),
        out_shape=outs,
        scratch_shapes=list(scratch),
        compiler_params=pltpu.CompilerParams(vmem_limit_bytes=limit),
        cost_estimate=pl.CostEstimate(flops=flops, bytes_accessed=1 << 20, transcendentals=0),
    )(*operands)


def shape(*dims, dtype=BF16):
    return jax.ShapeDtypeStruct(dims, dtype)


def cut_body(panel, out, sem):
    copy = pltpu.make_async_copy(panel.at[pl.ds(CUTS[0], SIZES[0])], out, sem)
    copy.start()
    copy.wait()


def first_body(rhs, inv, panel, base, low, piece, rhs_in, inv_in, sems):
    cut = pltpu.make_async_copy(panel.at[pl.ds(CUTS[1], SIZES[1])], piece, sems.at[0])

    @pl.when(column() < 2)
    def _():
        loads = [
            pltpu.make_async_copy(inv.at[lax.axis_index("core")], inv_in, sems.at[1]),
            pltpu.make_async_copy(rhs.at[:, pl.ds(0, NB)], rhs_in, sems.at[2]),
        ]
        for load in loads:
            load.start()
        for load in loads:
            load.wait()
        value = times_inverse(rhs_in[...], inv_in[...])
        base[...] = value
        low[...] = value.astype(BF16)

    cut.start()
    cut.wait()


def second_body(base, low, arrived, block, sent, inv, panel, *refs):
    quarters, cuts, inv_in, sems = refs[:4], refs[4:-2], refs[-2], refs[-1]
    copies = [
        pltpu.make_async_copy(panel.at[pl.ds(CUTS[k], SIZES[k])], out, sems.at[k])
        for k, out in enumerate(cuts, 2)
    ]
    part = NB // 4

    @pl.when(column() == 0)
    def _():
        for q in range(4):
            quarters[q][...] = low[pl.ds(q * part, part), :]

    @pl.when(column() == 1)
    def _():
        load = pltpu.make_async_copy(inv.at[1], inv_in, sems.at[0])
        load.start()
        below = jnp.where(lax.axis_index("row") == 0, block[...], sent[...])
        load.wait()
        product = dot_nt(arrived[...], below)
        value = (base[...] - times_inverse(product, inv_in[...])).astype(BF16)
        for q in range(4):
            quarters[q][...] = value[q * part : (q + 1) * part]

    for copy in copies:
        copy.start()
    for copy in copies:
        copy.wait()


def choose_body(place, *refs):
    given, outs = refs[:4], refs[4:]
    part = given[0].shape[0] // len(outs)
    for q in range(4):

        @pl.when(lax.axis_index(place) == q)
        def _():
            for i, out in enumerate(outs):
                out[...] = given[q][pl.ds(i * part, part), :]


def select_body(near, far, out):
    @pl.when(lax.axis_index("xh") == 0)
    def _():
        out[...] = near[...]

    @pl.when(lax.axis_index("xh") == 1)
    def _():
        out[...] = far[...]


def ring_body(own, up, down, far, out):
    y = lax.axis_index("y")
    out[y] = own[...]
    out[lax.rem(y + 1, 4)] = down[...]
    out[lax.rem(y + 2, 4)] = far[...]
    out[lax.rem(y + 3, 4)] = up[...]


def plane_body(own, up, down, far_a, far_b, out):
    z = lax.axis_index("z")
    for y in range(4):
        rows = slice(y * 32, y * 32 + 32)
        out[z, rows] = own[y]
        out[lax.rem(z + 1, 4), rows] = down[y]
        out[lax.rem(z + 2, 4), rows] = (far_a if y < 2 else far_b)[y % 2]
        out[lax.rem(z + 3, 4), rows] = up[y]


def lend_body(mine, theirs, out):
    out[...] = jnp.where(lax.axis_index("core") == lax.axis_index("row"), theirs[...], mine[...])


def finish_body(mine, theirs, lent, solved):
    row = lax.axis_index("row")
    solved[row] = jnp.where(lax.axis_index("core") == row, mine[...], theirs[...])
    solved[1 - row] = lent[...]


def update_body(group, mine, theirs, rhs, *refs):
    count = len(group)
    own, other = refs[:count], refs[count : 2 * count]
    sent = refs[2 * count] if group[0] == 0 else None
    out, rhs_in, out_buf, in_sems, out_sems = refs[-5:]
    row = lax.axis_index("row")
    same = lax.axis_index("core") == row
    tiles = [(k, a) for k, size in enumerate(SIZES[g] for g in group) for a in range(0, size, TILE)]
    loads, stores = [], []
    for t, (k, a) in enumerate(tiles):
        columns = pl.ds(CUTS[group[k]] + a, TILE)
        loads.append(pltpu.make_async_copy(rhs.at[:, columns], rhs_in.at[t], in_sems.at[t]))
        stores.append(pltpu.make_async_copy(out_buf.at[t], out.at[:, columns], out_sems.at[t]))
        loads[-1].start()
    left = jnp.where(same, mine[...], theirs[...])
    right = jnp.where(same, theirs[...], mine[...])
    for t, (k, a) in enumerate(tiles):
        rows = pl.ds(a, TILE)
        arrived = other[k][rows, :]
        if group[k] == 0:
            arrived = jnp.where((column() < 2), sent[rows, :], arrived)
        first = dot_nt(left, own[k][rows, :])
        second = dot_nt(right, arrived)
        if group[k] == 0:
            drop = (column() < 2) & (row >= column())
            first = jnp.where(drop, jnp.zeros_like(first), first)
            drop = (column() < 2) & (1 - row >= column())
            second = jnp.where(drop, jnp.zeros_like(second), second)
        loads[t].wait()
        out_buf[t] = rhs_in[t] - (first + second)
        stores[t].start()
    for store in stores:
        store.wait()


def update(group, mine, theirs, rhs, own, other, sent, before):
    width = sum(SIZES[g] for g in group)
    count = width // TILE
    operands = [mine, theirs, rhs] + [own[g] for g in group] + [other[g] for g in group]
    specs = [VMEM, VMEM, HBM] + [VMEM] * (2 * len(group))
    if group[0] == 0:
        operands.append(sent)
        specs.append(VMEM)
    aliases = {}
    if before is not None:
        aliases = {len(operands): 0}
        operands.append(before)
        specs.append(HBM)
    return pl.pallas_call(
        functools.partial(update_body, group),
        in_specs=specs,
        out_specs=HBM,
        out_shape=jax.ShapeDtypeStruct(rhs.shape, F32),
        input_output_aliases=aliases,
        scratch_shapes=[
            pltpu.VMEM((count, NB, TILE), F32),
            pltpu.VMEM((count, NB, TILE), F32),
            pltpu.SemaphoreType.DMA((count,)),
            pltpu.SemaphoreType.DMA((count,)),
        ],
        compiler_params=pltpu.CompilerParams(vmem_limit_bytes=(6 << 20) + 6 * NB * width * 4),
        cost_estimate=pl.CostEstimate(
            flops=4 * NB * NB * width, bytes_accessed=4 << 20, transcendentals=0
        ),
        name="update",
    )(*operands)


def move(value, axis, pairs):
    return lax.ppermute(value, axis, pairs)


def shift(value, axis, by):
    return move(value, axis, [(i, (i + by) % 4) for i in range(4)])


def toggle(value, axis, by):
    return move(value, axis, [(i, i ^ by) for i in range(4)])


def shards(panel, rhs, diag_inverse):
    swap = [(0, 1), (1, 0)]

    own = list(call(
        cut_body, [panel], [HBM], [shape(SIZES[0], NB)],
        [pltpu.SemaphoreType.DMA(())], room=11264,
    ))
    pairs = [(c, 64 + c) for c in range(2, 64)]
    other = [
        move(own[0], ALL, pairs + [(b, a) for a, b in pairs] + [(i, i) for i in (0, 1, 64, 65)])
    ]
    sent = move(own[0], ALL, [(1, 65), (65, 1)] + [(i, i) for i in range(128) if i not in (1, 65)])
    base, low, piece = call(
        first_body, [rhs, diag_inverse, panel], [HBM] * 3,
        [shape(NB, NB, dtype=F32), shape(NB, NB), shape(SIZES[1], NB)],
        [pltpu.VMEM((NB, NB), F32), pltpu.VMEM((NB, NB), BF16), pltpu.SemaphoreType.DMA((6,))],
        6 * NB**3, 12800,
    )
    own.append(piece)
    arrived = move(low, "core", swap)
    other.append(move(own[1], "row", swap))
    made = call(
        second_body, [base, low, arrived, own[0], sent, diag_inverse, panel],
        [VMEM] * 5 + [HBM] * 2,
        [shape(NB // 4, NB)] * 4 + [shape(size, NB) for size in SIZES[2:]],
        [pltpu.VMEM((NB, NB), BF16), pltpu.SemaphoreType.DMA((len(SIZES),))],
        8 * NB**3, 18432,
    )
    quarters, own = made[:4], own + list(made[4:])

    got = [toggle(quarters[q], "z", q) for q in range(1, 4)]
    parts = call(
        functools.partial(choose_body, "z"), [quarters[0]] + got, [VMEM] * 4,
        [shape(32, NB)] * 4,
    )
    got = [toggle(parts[q], "y", q) for q in range(1, 4)]
    (mine,) = call(
        functools.partial(choose_body, "y"), [parts[0]] + got, [VMEM] * 4,
        [shape(32, NB)],
    )
    along = move(mine, "xh", swap)
    for k in range(2, len(SIZES)):
        other.append(move(own[k], "row", swap))
    (mine,) = call(select_body, [mine, along], [VMEM] * 2, [shape(32, NB)])
    up, down, far = (shift(mine, "y", by) for by in (1, -1, 2))
    (line,) = call(ring_body, [mine, up, down, far], [VMEM] * 4, [shape(4, 32, NB)])
    up, down = shift(line, "z", 1), shift(line, "z", -1)
    far_a, far_b = shift(up[:2], "z", 1), shift(down[2:], "z", -1)
    (plane,) = call(
        plane_body, [line, up, down, far_a, far_b], [VMEM] * 5,
        [shape(4, 128, NB)],
    )
    mine = plane.reshape(NB, NB)
    theirs = move(mine, "core", swap)
    (lent,) = call(lend_body, [mine, theirs], [VMEM] * 2, [shape(NB, NB)])
    lent = move(lent, ("row", "xh"), [(0, 3), (3, 0), (1, 2), (2, 1)])
    updated = None
    for group in GROUPS:
        updated = update(group, mine, theirs, rhs, own, other, sent, updated)
    (solved,) = call(finish_body, [mine, theirs, lent], [VMEM] * 3, [shape(2, NB, NB)])
    return solved.reshape(2 * NB, NB), updated


def solution(mesh):
    split = Mesh(mesh.devices.reshape(2, 4, 4, 2, 2), ALL)
    return jax.shard_map(
        shards,
        mesh=split,
        in_specs=(P(COL, "row"), P("row", COL), P()),
        out_specs=(P(None, "row"), P("row", COL)),
        check_vma=False,
    )
```
